1024 devices in a mesh: dp: 4 (over z_hi, core), ctx: 32 (over x, z_lo), tensor: 8 (over y).
Axes of the slice: x: 8, y: 8, z: 8 (z_hi: 2, z_lo: 4; z = z_hi * 4 + z_lo), core: 2. Of those that a mesh axis runs over, the one named last changes fastest.
Arguments:
- query: bfloat16 [4, 4096, 128, 128], P('dp', 'ctx', 'tensor'), may hold values from -200 to 200
- key_value: bfloat16 [2, 4, 4096, 8, 128], P(None, 'dp', 'ctx'), may hold values from -7 to 7
- grad_out: bfloat16 [4, 4096, 128, 128], P('dp', 'ctx', 'tensor'), may hold values from -6 to 6
- doc_lengths: int32 [4, 16], P('dp'), may hold values from 1 to 640, 4096 in all within a row
- stretch_order: int32 [4, 32], P('dp'), may hold values from 0 to 31, each once within a row
- loss_mask: int32 [4, 4096], P('dp', 'ctx'), may hold values from 0 to 1
Outputs:
- attended: bfloat16 [4, 4096, 128, 128], P('dp', 'ctx', 'tensor')
- grad_query: bfloat16 [4, 4096, 128, 128], P('dp', 'ctx', 'tensor')
- grad_key_value: bfloat16 [2, 4, 4096, 8, 128], P(None, 'dp', 'ctx')
The draws below stay inside these ranges and needn't reach their ends.
Inputs may be any that keep to these rules, and one draw needn't show every extreme that they name: `doc_lengths`: each row sums to 4096 and its largest entry is 640. `stretch_order`: each row names every block index of its sequence once.
All inputs are finite; a program needn't handle non-finite values.
Results may differ from the reference program's by a relative error of at most 0.03.
Values may be sent and summed in bfloat16 or wider, within the bound.
No kernel may reach another device: no remote copies, remote signals or barrier semaphores. Data moves between devices by JAX's collectives and lax.ppermute only.
A program may use at most 32 MiB of HBM per device.

```python
import math
import jax
import jax.numpy as jnp
import numpy as np
from jax import lax

HEAD_DIM = 128
DOCS = 16
BATCH = 4
LENGTH = 4096
HEADS = 128
KV_HEADS = 8
MOST = 640
N_CTX = 32


def shared_keys(base_key):
    folded = jax.random.fold_in(base_key, 11)
    key_rows = jnp.clip(jax.random.normal(jax.random.fold_in(folded, 1), (BATCH, LENGTH, KV_HEADS, HEAD_DIM), jnp.float32), -6.0, 6.0)
    return key_rows


def draw_key_value(key, part):
    key_rows = shared_keys(key)
    values = jnp.clip(jax.random.normal(jax.random.fold_in(key, 41), (BATCH, LENGTH, KV_HEADS, HEAD_DIM), jnp.float32), -6.0, 6.0)
    return jnp.stack([key_rows, values]).astype(jnp.bfloat16)


def draw_query(key, part):
    queries = jnp.clip(jax.random.normal(jax.random.fold_in(key, 21), (BATCH, LENGTH, HEADS, HEAD_DIM), jnp.float32), -6.0, 6.0)
    return queries.astype(jnp.bfloat16)


def draw_loss_mask(key, part):
    total = BATCH * LENGTH
    flat = jnp.arange(total, dtype=jnp.int32)
    level = jax.random.randint(jax.random.fold_in(key, 62), (), 100, 1001)
    member_level = jax.random.randint(jax.random.fold_in(key, 63), (BATCH,), 75, 101)
    member_of = flat // LENGTH
    member_factor = jnp.sum(jnp.where(member_of[:, None] == jnp.arange(BATCH, dtype=jnp.int32)[None, :], member_level[None, :], 0), axis=1)
    profile = 200 + 700 * flat // total
    threshold = level * member_factor * profile // 100000
    rolled = jax.random.randint(jax.random.fold_in(key, 61), (total,), 0, 1000)
    return (rolled < threshold).astype(jnp.int32).reshape(BATCH, LENGTH)


def steps_of(own_key, dims, shards, low, high):
    level = 1.0
    for position, shards_of in shards:
        draws = jax.random.uniform(jax.random.fold_in(jax.random.fold_in(own_key, 6), position), (shards_of,), jnp.float32, low / len(shards), high / len(shards))
        level = level * jnp.repeat(jnp.exp(draws), dims[position] // shards_of).reshape((-1,) + (1,) * (len(dims) - 1 - position))
    return level


def length_profile(count, total, reach, slope):
    weights = [(1 << 20) // math.isqrt(grade ** slope) + 1 for grade in range(2, count + 1)]
    spare, given = total - reach - (count - 1), [1] * (count - 1)
    while spare > 0:
        movable = [i for i in range(count - 1) if given[i] < reach]
        pool, remaining = sum([weights[i] for i in movable]), spare
        for i in movable:
            more = min(reach - given[i], max(1, remaining * weights[i] // pool), spare)
            given[i] = given[i] + more
            spare = spare - more
    return np.array([reach] + given)


def ragged(key, count, total, most, slope):
    if count == 2:
        one = jax.random.randint(key, (), max(1, total - most), min(most, total - 1) + 1)
        return jnp.stack([one, total - one])
    tallies = jnp.asarray(length_profile(count, total, most, slope), jnp.int32)
    couples = (count - 1) // 2
    giver, taker = tallies[1:1 + 2 * couples:2], tallies[2:2 + 2 * couples:2]
    slack = jnp.minimum(giver - 1, most - taker)
    shifted = jax.random.randint(jax.random.fold_in(key, 1), (couples,), 0, 1 << 20) % (slack + 1)
    tallies = tallies.at[1:1 + 2 * couples:2].set(giver - shifted).at[2:2 + 2 * couples:2].set(taker + shifted)
    return tallies[jax.random.permutation(jax.random.fold_in(key, 2), count)]


def noise(rng, shape, scale, reach, shards=(), kind=jnp.bfloat16):
    array = scale * jax.random.normal(rng, shape, jnp.float32)
    if shards:
        array = array * steps_of(rng, shape, shards, -0.22, 0.18)
    return jnp.clip(array, -reach, reach).astype(kind)


def setup_inputs(seed: int = 0) -> dict:
    key_of = jax.random.split(jax.random.key(seed), 7)
    query = draw_query(jax.random.fold_in(key_of[6], 71), 0)
    key_value = draw_key_value(jax.random.fold_in(key_of[6], 71), 0)
    grad_out = noise(key_of[2], (BATCH, LENGTH, HEADS, HEAD_DIM), 1.0, 6.0, ((0, 4), (1, 32), (2, 8)))
    doc_lengths = jax.vmap(lambda own: ragged(own, DOCS, LENGTH, MOST, 2))(jax.random.split(key_of[3], BATCH)).reshape((BATCH, DOCS)).astype(jnp.int32)
    stretch_order = jax.vmap(lambda own: jax.random.permutation(own, N_CTX))(jax.random.split(key_of[4], BATCH)).reshape((BATCH, N_CTX)).astype(jnp.int32)
    loss_mask = draw_loss_mask(jax.random.fold_in(key_of[6], 71), 0)
    return dict(query=query, key_value=key_value, grad_out=grad_out, doc_lengths=doc_lengths, stretch_order=stretch_order, loss_mask=loss_mask)


def batched(left_side, right_side, pattern):
    return jnp.einsum(pattern, left_side.astype(jnp.float32), right_side.astype(jnp.float32), precision=lax.Precision.HIGHEST)

def reference(query, key_value, grad_out, doc_lengths, stretch_order, loss_mask):
    seq_count = query.shape[0]
    length = query.shape[1]
    head_count = query.shape[2]
    head_width = query.shape[3]
    kv_count = key_value.shape[3]
    group_size = head_count // kv_count
    shard_rows = length // N_CTX
    window = (MOST - 1 + shard_rows - 1) // shard_rows
    margin = window * shard_rows
    span_rows = margin + shard_rows
    factor = 1.0 / math.sqrt(head_width)
    counted = jnp.maximum(jnp.sum(loss_mask.astype(jnp.float32)), 1.0)
    weight = seq_count * length / counted
    ordinal = jnp.arange(length, dtype=jnp.int32)
    window_rows = jnp.arange(N_CTX, dtype=jnp.int32)[:, None] * shard_rows + jnp.arange(span_rows, dtype=jnp.int32)[None, :]
    key_places = window_rows - margin
    query_places = ordinal.reshape(N_CTX, shard_rows)
    flat_rows = window_rows.reshape(-1)
    attended_list = []
    query_list = []
    key_list = []
    value_list = []
    for member in range(seq_count):
        order_row = stretch_order[member]
        places = order_row[ordinal // shard_rows] * shard_rows + ordinal % shard_rows
        holder = jnp.zeros((N_CTX,), jnp.int32).at[order_row].set(jnp.arange(N_CTX, dtype=jnp.int32))
        sources = holder[ordinal // shard_rows] * shard_rows + ordinal % shard_rows
        bounds = jnp.cumsum(doc_lengths[member])
        doc_ids = lax.optimization_barrier(jnp.sum((bounds[None, :] <= ordinal[:, None]).astype(jnp.int32), axis=1))
        padded_docs = jnp.concatenate([jnp.full((margin,), -1, jnp.int32), doc_ids])
        visible = (doc_ids.reshape(N_CTX, shard_rows)[:, :, None] == padded_docs[window_rows][:, None, :]) & (key_places[:, None, :] <= query_places[:, :, None])
        scaled = (grad_out[member].astype(jnp.float32) * loss_mask[member][:, None, None].astype(jnp.float32) * weight).astype(jnp.bfloat16)
        queries_all = query[member][sources]
        upstream_all = scaled[sources]
        padding = jnp.zeros((2, margin, kv_count, head_width), key_value.dtype)
        pair_padded = jnp.concatenate([padding, key_value[:, member][:, sources]], axis=1)
        pair_window = pair_padded[:, window_rows]

        def per_head(head_index):
            queries = lax.dynamic_index_in_dim(queries_all, head_index, 1, keepdims=False).reshape(N_CTX, shard_rows, head_width)
            upstream = lax.dynamic_index_in_dim(upstream_all, head_index, 1, keepdims=False).reshape(N_CTX, shard_rows, head_width)
            group_index = head_index // group_size
            key_rows = lax.dynamic_index_in_dim(pair_window[0], group_index, 2, keepdims=False)
            values = lax.dynamic_index_in_dim(pair_window[1], group_index, 2, keepdims=False)
            scores = batched(queries, key_rows, 'cqd,ckd->cqk') * factor
            scores = jnp.where(visible, scores, -1e+30)
            highest = lax.optimization_barrier(jnp.max(scores, axis=2, keepdims=True))
            exponent = jnp.where(visible, jnp.exp(scores - highest), 0.0)
            probabilities = exponent / lax.optimization_barrier(jnp.sum(exponent, axis=2, keepdims=True))
            probs_low = probabilities.astype(jnp.bfloat16)
            output = batched(probs_low, values, 'cqk,ckd->cqd').astype(jnp.bfloat16)
            row_delta = lax.optimization_barrier(jnp.sum(upstream.astype(jnp.float32) * output.astype(jnp.float32), axis=2, keepdims=True))
            prob_grad = batched(upstream, values, 'cqd,ckd->cqk')
            score_grad = (probabilities * (prob_grad - row_delta)).astype(jnp.bfloat16)
            query_grad = (batched(score_grad, key_rows, 'cqk,ckd->cqd') * factor).astype(jnp.bfloat16)
            key_part = batched(score_grad, queries, 'cqk,cqd->ckd') * factor
            value_part = batched(probs_low, upstream, 'cqk,cqd->ckd')
            empty = jnp.zeros((margin + length, head_width), jnp.float32)
            key_grad = empty.at[flat_rows].add(key_part.reshape(-1, head_width))[margin:]
            value_grad = empty.at[flat_rows].add(value_part.reshape(-1, head_width))[margin:]
            return (output.reshape(length, head_width), query_grad.reshape(length, head_width), key_grad, value_grad)
        outputs, query_grads, key_grads, value_grads = lax.map(per_head, jnp.arange(head_count, dtype=jnp.int32))
        attended_list.append(jnp.transpose(outputs[:, places], (1, 0, 2)))
        query_list.append(jnp.transpose(query_grads[:, places], (1, 0, 2)))
        key_sum = lax.optimization_barrier(jnp.sum(key_grads.reshape(kv_count, group_size, length, head_width), axis=1))[:, places]
        value_sum = lax.optimization_barrier(jnp.sum(value_grads.reshape(kv_count, group_size, length, head_width), axis=1))[:, places]
        key_list.append(jnp.transpose(key_sum, (1, 0, 2)))
        value_list.append(jnp.transpose(value_sum, (1, 0, 2)))
    attended = jnp.stack(attended_list)
    grad_query = jnp.stack(query_list)
    grad_key_value = jnp.stack([jnp.stack(key_list), jnp.stack(value_list)]).astype(jnp.bfloat16)
    return (attended, grad_query, grad_key_value)
```

```python
import functools
import math

import jax
import jax.numpy as jnp
from jax import lax
from jax.experimental import pallas as pl
from jax.experimental.pallas import tpu as pltpu
from jax.sharding import Mesh
from jax.sharding import PartitionSpec as P

CTX = ("ctx_0", "ctx_1")
DP = ("dp_0", "dp_1")
WORLD = ("ctx_0", "ctx_1", "tensor")

FLOOR_SCORE = -1e30
SUB = 8

VMEM = pl.BlockSpec(memory_space=pltpu.VMEM)
SMEM = pl.BlockSpec(memory_space=pltpu.SMEM)


def fill_holders(holders, order_ref, count, window):
    for i in range(window):
        holders[i] = -1
        holders[count + window + i] = -1
    for c in range(count):
        holders[order_ref[0, c] + window] = c


def select_kernel(order_ref, got_ref, out_ref, count_ref, holders, *, count, window):
    fill_holders(holders, order_ref, count, window)
    for d in range(count):
        own = order_ref[0, d]
        for j in range(window):
            source = jnp.maximum(holders[own + j], 0)
            out_ref[d, j] = got_ref[source, :SUB]
    total = jnp.zeros((SUB, got_ref.shape[2]), jnp.float32)
    for c in range(count):
        total = total + got_ref[c, SUB:].astype(jnp.float32)
    count_ref[...] = total


def reduce_kernel(order_ref, total_ref, got_ref, out_ref, holders, *, count, window, tokens):
    fill_holders(holders, order_ref, count, window)
    weight = tokens / jnp.maximum(total_ref[...], 1.0)
    copies = out_ref.shape[1]
    for c in range(count):
        own = order_ref[0, c]
        summed = got_ref[c, window].astype(jnp.float32)
        for j in range(window):
            source = holders[own + 2 * window - j]
            term = got_ref[jnp.maximum(source, 0), j].astype(jnp.float32)
            summed = summed + jnp.where(source >= 0, term, 0.0)
        piece = (summed * weight).astype(out_ref.dtype)
        for g in range(copies):
            out_ref[c, g] = piece


def attend_kernel(
    me_ref,
    order_ref,
    length_ref,
    q_ref,
    up_ref,
    own_ref,
    got_ref,
    att_ref,
    gq_ref,
    part_ref,
    keys,
    values,
    keys_t,
    values_t,
    grad_k,
    grad_v,
    *,
    window,
    heads,
    chunk,
):
    pieces = own_ref.shape[0]
    half = pieces // 2
    rows, width = q_ref.shape
    block = half * SUB
    prior = window * block
    span = prior + block
    factor = 1.0 / math.sqrt(width)
    own = order_ref[0, me_ref[0]]
    docs = length_ref.shape[1]

    for j in range(window):
        keys[j * block : (j + 1) * block] = got_ref[:half, j].reshape(block, width)
        values[j * block : (j + 1) * block] = got_ref[half:, j].reshape(block, width)
    keys[prior:] = own_ref[:half, :SUB].reshape(block, width)
    values[prior:] = own_ref[half:, :SUB].reshape(block, width)
    keys_t[...] = keys[...].astype(jnp.float32).T.astype(jnp.bfloat16)
    values_t[...] = values[...].astype(jnp.float32).T.astype(jnp.bfloat16)
    grad_k[...] = jnp.zeros_like(grad_k)
    grad_v[...] = jnp.zeros_like(grad_v)

    bounds = []
    running = jnp.int32(0)
    for j in range(docs):
        running = running + length_ref[0, j]
        bounds.append(running)

    nt = (((1,), (1,)), ((), ()))
    nn = (((1,), (0,)), ((), ()))

    def dot(a, b, dims):
        return lax.dot_general(a, b, dims, preferred_element_type=jnp.float32)

    def step(c, _):
        first = pl.multiple_of(c * chunk, chunk)
        here = pl.ds(first, chunk)
        q = q_ref[here, :]
        up = up_ref[here, :]
        token = (first + lax.broadcasted_iota(jnp.int32, (1, chunk), 1)) // heads
        place = own * block + token
        start = jnp.zeros((1, chunk), jnp.int32)
        for bound in bounds:
            start = jnp.where(bound <= place, bound, start)
        low = start - (own - window) * block
        high = token + prior

        scores = dot(keys[...], q, nt)
        index = lax.broadcasted_iota(jnp.int32, (span, chunk), 0)
        visible = (index >= low) & (index <= high)
        scores = jnp.where(visible, scores, FLOOR_SCORE)
        highest = jnp.max(scores, axis=0, keepdims=True)
        exponent = jnp.exp((scores - highest) * factor)
        probs = exponent * (1.0 / jnp.sum(exponent, axis=0, keepdims=True))
        probs_low = probs.astype(jnp.bfloat16)
        att = dot(values_t[...], probs_low, nn)
        att_ref[here, :] = att.T.astype(att_ref.dtype)
        prob_grad = dot(values[...], up, nt)
        delta = jnp.sum(probs * prob_grad, axis=0, keepdims=True)
        score_grad = (probs * (prob_grad - delta)).astype(jnp.bfloat16)
        gq = dot(keys_t[...], score_grad, nn)
        gq_ref[here, :] = gq.T * factor
        grad_v[...] += dot(probs_low, up, nn)
        grad_k[...] += dot(score_grad, q, nn)
        return 0

    lax.fori_loop(0, rows // chunk, step, 0)

    for j in range(window + 1):
        part_ref[:half, j] = (
            (grad_k[j * block : (j + 1) * block] * factor)
            .astype(part_ref.dtype)
            .reshape(half, SUB, width)
        )
        part_ref[half:, j] = (
            grad_v[j * block : (j + 1) * block]
            .astype(part_ref.dtype)
            .reshape(half, SUB, width)
        )


def exchange(x, axes):
    return lax.all_to_all(x, axes, 0, 0, tiled=True)


def local(query, key_value, grad_out, doc_lengths, stretch_order, loss_mask):
    shard_rows, local_heads, head_width = query.shape[1:]
    kv_heads = key_value.shape[3]
    count = lax.axis_size(CTX)
    length = shard_rows * count
    longest = length * 5 // 32
    window = (longest - 1 + shard_rows - 1) // shard_rows
    rows = shard_rows * local_heads
    tokens = float(lax.axis_size(DP) * query.shape[0] * length)
    pieces = 2 * shard_rows // SUB
    assert pieces == count

    own_pair = lax.dynamic_index_in_dim(
        key_value[:, 0], lax.axis_index("tensor"), 2, keepdims=False
    ).reshape(pieces, SUB, head_width)
    counted = jnp.sum(loss_mask).astype(jnp.bfloat16)
    spread = jnp.concatenate(
        [own_pair, jnp.broadcast_to(counted, (pieces, SUB, head_width))], axis=1
    )
    got = exchange(spread, CTX)

    queries = query.reshape(rows, head_width)
    upstream = jnp.where(
        loss_mask[0][:, None, None] != 0, grad_out[0], jnp.zeros((), grad_out.dtype)
    ).reshape(rows, head_width)

    chosen, total = pl.pallas_call(
        functools.partial(select_kernel, count=count, window=window),
        out_shape=(
            jax.ShapeDtypeStruct((count, window, SUB, head_width), jnp.bfloat16),
            jax.ShapeDtypeStruct((SUB, head_width), jnp.float32),
        ),
        in_specs=[SMEM, VMEM],
        out_specs=(VMEM, VMEM),
        scratch_shapes=[pltpu.SMEM((count + 2 * window,), jnp.int32)],
        cost_estimate=pl.CostEstimate(flops=2_000_000, bytes_accessed=500_000, transcendentals=0),
        compiler_params=pltpu.CompilerParams(vmem_limit_bytes=4 * 1024 * 1024),
        name="select",
    )(stretch_order, got)
    fetched = exchange(chosen.reshape(count, window * SUB, head_width), CTX)
    fetched = fetched.reshape(count, window, SUB, head_width)

    pair = [(0, 1), (1, 0)]
    total = total + lax.ppermute(total, "dp_1", pair)
    total = total + lax.ppermute(total, "dp_0", pair)

    me = lax.axis_index(CTX).reshape(1).astype(jnp.int32)
    span = (window + 1) * shard_rows
    attended, grad_rows, parts = pl.pallas_call(
        functools.partial(attend_kernel, window=window, heads=local_heads, chunk=256),
        out_shape=(
            jax.ShapeDtypeStruct((rows, head_width), jnp.bfloat16),
            jax.ShapeDtypeStruct((rows, head_width), jnp.float32),
            jax.ShapeDtypeStruct((count, window + 1, SUB, head_width), jnp.bfloat16),
        ),
        in_specs=[SMEM, SMEM, SMEM, VMEM, VMEM, VMEM, VMEM],
        out_specs=(VMEM, VMEM, VMEM),
        scratch_shapes=[
            pltpu.VMEM((span, head_width), jnp.bfloat16),
            pltpu.VMEM((span, head_width), jnp.bfloat16),
            pltpu.VMEM((head_width, span), jnp.bfloat16),
            pltpu.VMEM((head_width, span), jnp.bfloat16),
            pltpu.VMEM((span, head_width), jnp.float32),
            pltpu.VMEM((span, head_width), jnp.float32),
        ],
        cost_estimate=pl.CostEstimate(
            flops=12 * rows * span * head_width, bytes_accessed=4_000_000, transcendentals=rows * span
        ),
        compiler_params=pltpu.CompilerParams(vmem_limit_bytes=24 * 1024 * 1024),
        name="attend",
    )(me, stretch_order, doc_lengths, queries, upstream, spread, fetched)

    met = exchange(parts.reshape(count, (window + 1) * SUB, head_width), CTX)
    summed = pl.pallas_call(
        functools.partial(reduce_kernel, count=count, window=window, tokens=tokens),
        out_shape=jax.ShapeDtypeStruct((count, kv_heads, SUB, head_width), jnp.bfloat16),
        in_specs=[SMEM, VMEM, VMEM],
        out_specs=VMEM,
        scratch_shapes=[pltpu.SMEM((count + 2 * window,), jnp.int32)],
        cost_estimate=pl.CostEstimate(flops=2_000_000, bytes_accessed=1_000_000, transcendentals=0),
        compiler_params=pltpu.CompilerParams(vmem_limit_bytes=4 * 1024 * 1024),
        name="reduce",
    )(stretch_order, total, met.reshape(count, window + 1, SUB, head_width))
    home = exchange(summed.reshape(count * kv_heads, SUB, head_width), WORLD)
    home = home.reshape(2, pieces // 2, kv_heads, SUB, head_width)
    grad_key_value = jnp.transpose(home, (0, 1, 3, 2, 4)).reshape(
        2, 1, shard_rows, kv_heads, head_width
    )

    weight = tokens / jnp.maximum(total[0, 0], 1.0)
    grad_query = (grad_rows * weight).astype(jnp.bfloat16).reshape(query.shape)
    return (attended.reshape(query.shape), grad_query, grad_key_value)


def solution(mesh):
    torus = Mesh(
        mesh.devices.reshape(2, 2, 8, 4, mesh.shape["tensor"]),
        ("dp_0", "dp_1", "ctx_0", "ctx_1", "tensor"),
    )
    placed = (
        P(DP, CTX, "tensor", None),
        P(None, DP, CTX, None, None),
        P(DP, CTX, "tensor", None),
        P(DP, None),
        P(DP, None),
        P(DP, CTX),
    )
    return jax.shard_map(
        local,
        mesh=torus,
        in_specs=placed,
        out_specs=(
            P(DP, CTX, "tensor", None),
            P(DP, CTX, "tensor", None),
            P(None, DP, CTX, None, None),
        ),
        check_vma=False,
    )
```

```python
import functools
import math

import jax
import jax.numpy as jnp
from jax import lax
from jax.experimental import pallas as pl
from jax.experimental.pallas import tpu as pltpu
from jax.sharding import Mesh
from jax.sharding import PartitionSpec as P

CTX = ("ctx_0", "ctx_1")
DP = ("dp_0", "dp_1")
WORLD = ("ctx_0", "ctx_1", "tensor")

FLOOR_SCORE = -1e30
SUB = 8
CHUNK = 512
UNROLL = 1

VMEM = pl.BlockSpec(memory_space=pltpu.VMEM)
SMEM = pl.BlockSpec(memory_space=pltpu.SMEM)


def fill_holders(holders, order_ref, count, window):
    for i in range(window):
        holders[i] = -1
        holders[count + window + i] = -1
    for c in range(count):
        holders[order_ref[0, c] + window] = c


def spread_kernel(head_ref, mask_ref, rows_ref, out_ref, *, heads):
    pieces = out_ref.shape[0]
    group = 256
    tokens = group // heads
    row = lax.broadcasted_iota(jnp.int32, (tokens, group), 1)
    token = lax.broadcasted_iota(jnp.int32, (tokens, group), 0)
    chosen = (row == token * heads + head_ref[0]).astype(jnp.float32).astype(jnp.bfloat16)
    each = tokens // SUB
    counted = jnp.sum(mask_ref[...].astype(jnp.float32), axis=1, keepdims=True)
    counted = jnp.broadcast_to(counted, (SUB, out_ref.shape[2])).astype(out_ref.dtype)
    for n in range(pieces // each):
        picked = jnp.dot(
            chosen, rows_ref[n * group : (n + 1) * group], preferred_element_type=jnp.float32
        ).astype(out_ref.dtype)
        for e in range(each):
            out_ref[n * each + e, :SUB] = picked[e * SUB : (e + 1) * SUB]
            out_ref[n * each + e, SUB:] = counted


def select_kernel(order_ref, got_ref, out_ref, count_ref, holders, *, count, window):
    fill_holders(holders, order_ref, count, window)
    total = jnp.zeros((SUB, got_ref.shape[2]), jnp.float32)
    for c in range(count):
        total = total + got_ref[c, SUB:].astype(jnp.float32)
    count_ref[...] = total
    for d in range(count):
        own = order_ref[0, d]
        for j in range(window):
            source = jnp.maximum(holders[own + j], 0)
            out_ref[d, j] = got_ref[source, :SUB]


def reduce_kernel(
    order_ref, count_ref, got_ref, rows_ref, out_ref, grad_ref, holders, *, count, window, groups, tokens
):
    fill_holders(holders, order_ref, count, window)
    total = count_ref[:1]
    for k in range(groups - 1):
        other = got_ref[k, window + 1].astype(jnp.float32)
        total = total + other[:1] * 64.0 + other[4:5]
    weight = tokens / jnp.maximum(total, 1.0)
    copies = out_ref.shape[1]
    for c in range(count):
        own = order_ref[0, c]
        summed = got_ref[c, window].astype(jnp.float32)
        for j in range(window):
            source = holders[own + 2 * window - j]
            term = got_ref[jnp.maximum(source, 0), j].astype(jnp.float32)
            summed = summed + jnp.where(source >= 0, term, 0.0)
        piece = (summed * weight).astype(out_ref.dtype)
        for g in range(copies):
            out_ref[c, g] = piece
    grad_ref[...] = (rows_ref[...] * weight).astype(grad_ref.dtype)


def attend_kernel(
    me_ref,
    order_ref,
    length_ref,
    mask_ref,
    q_ref,
    up_ref,
    own_ref,
    got_ref,
    count_ref,
    att_ref,
    gq_ref,
    part_ref,
    keys,
    values,
    keys_t,
    values_t,
    grad_k,
    grad_v,
    *,
    window,
    heads,
    chunk,
    unroll,
):
    pieces = own_ref.shape[0]
    half = pieces // 2
    rows, width = q_ref.shape
    block = half * SUB
    prior = window * block
    span = prior + block
    factor = 1.0 / math.sqrt(width)
    own = order_ref[0, me_ref[0]]
    docs = length_ref.shape[1]

    lane = lax.broadcasted_iota(jnp.int32, (1, width), 1)
    first = jnp.where(lane == docs, -span, 0)
    last = jnp.zeros((1, width), jnp.int32)
    running = jnp.int32(0)
    for d in range(docs):
        first = jnp.where(lane == d, running, first)
        running = running + length_ref[0, d]
        last = jnp.where(lane == d, running, last)

    for j in range(window):
        keys[j * block : (j + 1) * block, :width] = got_ref[:half, j].reshape(block, width)
        values[j * block : (j + 1) * block] = got_ref[half:, j].reshape(block, width)
    keys[prior:, :width] = own_ref[:half, :SUB].reshape(block, width)
    values[prior:] = own_ref[half:, :SUB].reshape(block, width)
    spot = (own - window) * block + lax.broadcasted_iota(jnp.int32, (span, width), 0)
    within = (spot >= first) & (spot < last)
    keys[:, width:] = jnp.where(within, 1.0, 0.0).astype(jnp.bfloat16)
    keys_t[...] = keys[:, :width].astype(jnp.float32).T.astype(jnp.bfloat16)
    values_t[...] = values[...].astype(jnp.float32).T.astype(jnp.bfloat16)
    grad_k[...] = jnp.zeros_like(grad_k)
    grad_v[...] = jnp.zeros_like(grad_v)

    nt = (((1,), (1,)), ((), ()))
    nn = (((1,), (0,)), ((), ()))

    def dot(a, b, dims):
        return lax.dot_general(a, b, dims, preferred_element_type=jnp.float32)

    assert heads & (heads - 1) == 0

    def token_of(row):
        return lax.shift_right_logical(row, heads.bit_length() - 1)

    def step(c, _):
        start = pl.multiple_of(c * chunk, chunk)
        here = pl.ds(start, chunk)
        q = q_ref[here, :]
        place = own * block + token_of(start + lax.broadcasted_iota(jnp.int32, (chunk, width), 0))
        within = (place >= first) & (place < last)
        barred = jnp.where(within, 0.0, FLOOR_SCORE).astype(jnp.bfloat16)
        token = token_of(start)
        up = jnp.concatenate(
            [
                jnp.where(
                    mask_ref[0, token + i] != 0,
                    up_ref[pl.ds(start + i * heads, heads), :].astype(jnp.float32),
                    0.0,
                ).astype(jnp.bfloat16)
                for i in range(chunk // heads)
            ],
            axis=0,
        )

        scores = dot(keys[...], jnp.concatenate([q, barred], axis=1), nt)
        index = lax.broadcasted_iota(jnp.int32, (block, chunk), 0)
        column = token_of(start + lax.broadcasted_iota(jnp.int32, (block, chunk), 1))
        here_scores = jnp.where(index <= column, scores[prior:], FLOOR_SCORE)
        scores = jnp.concatenate([scores[:prior], here_scores], axis=0)
        highest = jnp.max(scores, axis=0, keepdims=True)
        exponent = jnp.exp2((scores - highest) * (factor / math.log(2.0)))
        probs = exponent * (1.0 / jnp.sum(exponent, axis=0, keepdims=True))
        probs_low = probs.astype(jnp.bfloat16)
        prob_grad = dot(values[...], up, nt)
        att = dot(values_t[...], probs_low, nn)
        att_ref[here, :] = att.T.astype(att_ref.dtype)
        delta = jnp.sum(probs * prob_grad, axis=0, keepdims=True)
        score_grad = (probs * (prob_grad - delta)).astype(jnp.bfloat16)
        gq = dot(keys_t[...], score_grad, nn)
        gq_ref[here, :] = gq.T * factor
        grad_v[...] += dot(probs_low, up, nn)
        grad_k[...] += dot(score_grad, q, nn)
        return 0

    lax.fori_loop(0, rows // chunk, step, 0, unroll=unroll)

    for j in range(window + 1):
        part_ref[:half, j] = (
            (grad_k[j * block : (j + 1) * block] * factor)
            .astype(part_ref.dtype)
            .reshape(half, SUB, width)
        )
        part_ref[half:, j] = (
            grad_v[j * block : (j + 1) * block]
            .astype(part_ref.dtype)
            .reshape(half, SUB, width)
        )
    high = jnp.floor(count_ref[...] * (1.0 / 64.0))
    low = count_ref[...] - high * 64.0
    upper = lax.broadcasted_iota(jnp.int32, (SUB, width), 0) < 4
    halves = jnp.where(upper, high, low).astype(part_ref.dtype)
    for i in range(pieces):
        part_ref[i, window + 1] = halves


def limit(mib):
    return pltpu.CompilerParams(vmem_limit_bytes=mib * 1024 * 1024)


def exchange(x, axes):
    return lax.all_to_all(x, axes, 0, 0, tiled=True)


def local(query, key_value, grad_out, doc_lengths, stretch_order, loss_mask):
    shard_rows, local_heads, head_width = query.shape[1:]
    kv_heads = key_value.shape[3]
    count = lax.axis_size(CTX)
    length = shard_rows * count
    longest = length * 5 // 32
    window = (longest - 1 + shard_rows - 1) // shard_rows
    rows = shard_rows * local_heads
    tokens = float(lax.axis_size(DP) * query.shape[0] * length)
    pieces = 2 * shard_rows // SUB
    assert pieces == count

    head = lax.axis_index("tensor").reshape(1).astype(jnp.int32)
    spread = pl.pallas_call(
        functools.partial(spread_kernel, heads=kv_heads),
        out_shape=jax.ShapeDtypeStruct((pieces, 2 * SUB, head_width), jnp.bfloat16),
        in_specs=[SMEM, VMEM, VMEM],
        out_specs=VMEM,
        compiler_params=limit(4),
        cost_estimate=pl.CostEstimate(flops=20_000_000, bytes_accessed=700_000, transcendentals=0),
        name="spread",
    )(head, loss_mask, key_value.reshape(2 * shard_rows * kv_heads, head_width))
    got = exchange(spread, CTX)

    chosen, counted = pl.pallas_call(
        functools.partial(select_kernel, count=count, window=window),
        out_shape=(
            jax.ShapeDtypeStruct((count, window, SUB, head_width), jnp.bfloat16),
            jax.ShapeDtypeStruct((SUB, head_width), jnp.float32),
        ),
        in_specs=[SMEM, VMEM],
        out_specs=(VMEM, VMEM),
        scratch_shapes=[pltpu.SMEM((count + 2 * window,), jnp.int32)],
        compiler_params=limit(4),
        cost_estimate=pl.CostEstimate(flops=2_000_000, bytes_accessed=500_000, transcendentals=0),
        name="select",
    )(stretch_order, got)
    groups = lax.axis_size(DP)
    pairs = [
        (a * count + c, (a ^ (1 + c % (groups - 1))) * count + c)
        for a in range(groups)
        for c in range(count)
    ]
    heard = lax.ppermute(counted, DP + CTX, pairs)
    fetched = exchange(chosen.reshape(count, window * SUB, head_width), CTX)
    fetched = fetched.reshape(count, window, SUB, head_width)

    me = lax.axis_index(CTX).reshape(1).astype(jnp.int32)
    span = (window + 1) * shard_rows
    attended, grad_rows, parts = pl.pallas_call(
        functools.partial(
            attend_kernel, window=window, heads=local_heads, chunk=CHUNK, unroll=UNROLL
        ),
        out_shape=(
            jax.ShapeDtypeStruct((rows, head_width), jnp.bfloat16),
            jax.ShapeDtypeStruct((rows, head_width), jnp.float32),
            jax.ShapeDtypeStruct((count, window + 2, SUB, head_width), jnp.bfloat16),
        ),
        in_specs=[SMEM, SMEM, SMEM, SMEM, VMEM, VMEM, VMEM, VMEM, VMEM],
        out_specs=(VMEM, VMEM, VMEM),
        scratch_shapes=[
            pltpu.VMEM((span, 2 * head_width), jnp.bfloat16),
            pltpu.VMEM((span, head_width), jnp.bfloat16),
            pltpu.VMEM((head_width, span), jnp.bfloat16),
            pltpu.VMEM((head_width, span), jnp.bfloat16),
            pltpu.VMEM((span, head_width), jnp.float32),
            pltpu.VMEM((span, head_width), jnp.float32),
        ],
        compiler_params=limit(24),
        cost_estimate=pl.CostEstimate(
            flops=12 * rows * span * head_width, bytes_accessed=4_000_000, transcendentals=rows * span
        ),
        name="attend",
    )(
        me,
        stretch_order,
        doc_lengths,
        loss_mask,
        query.reshape(rows, head_width),
        grad_out.reshape(rows, head_width),
        spread,
        fetched,
        heard,
    )

    met = exchange(parts.reshape(count, (window + 2) * SUB, head_width), CTX)
    summed, grad_query = pl.pallas_call(
        functools.partial(
            reduce_kernel, count=count, window=window, groups=groups, tokens=tokens
        ),
        out_shape=(
            jax.ShapeDtypeStruct((count, kv_heads, SUB, head_width), jnp.bfloat16),
            jax.ShapeDtypeStruct((rows, head_width), jnp.bfloat16),
        ),
        in_specs=[SMEM, VMEM, VMEM, VMEM],
        out_specs=(VMEM, VMEM),
        scratch_shapes=[pltpu.SMEM((count + 2 * window,), jnp.int32)],
        compiler_params=limit(6),
        cost_estimate=pl.CostEstimate(flops=2_000_000, bytes_accessed=1_000_000, transcendentals=0),
        name="reduce",
    )(stretch_order, counted, met.reshape(count, window + 2, SUB, head_width), grad_rows)
    home = exchange(summed.reshape(count * kv_heads, SUB, head_width), WORLD)
    home = home.reshape(2, pieces // 2, kv_heads, SUB, head_width)
    grad_key_value = jnp.transpose(home, (0, 1, 3, 2, 4)).reshape(
        2, 1, shard_rows, kv_heads, head_width
    )
    return (attended.reshape(query.shape), grad_query.reshape(query.shape), grad_key_value)


def solution(mesh):
    torus = Mesh(
        mesh.devices.reshape(2, 2, 8, 4, mesh.shape["tensor"]),
        ("dp_0", "dp_1", "ctx_0", "ctx_1", "tensor"),
    )
    placed = (
        P(DP, CTX, "tensor", None),
        P(None, DP, CTX, None, None),
        P(DP, CTX, "tensor", None),
        P(DP, None),
        P(DP, None),
        P(DP, CTX),
    )
    return jax.shard_map(
        local,
        mesh=torus,
        in_specs=placed,
        out_specs=(
            P(DP, CTX, "tensor", None),
            P(DP, CTX, "tensor", None),
            P(None, DP, CTX, None, None),
        ),
        check_vma=False,
    )
```

```python
import functools
import math

import jax
import jax.numpy as jnp
from jax import lax
from jax.experimental import pallas as pl
from jax.experimental.pallas import tpu as pltpu
from jax.sharding import Mesh
from jax.sharding import PartitionSpec as P


CTX = ("ctx_0", "ctx_1")
DP = ("dp_0", "dp_1")
WORLD = ("ctx_0", "ctx_1", "tensor")

FLOOR_SCORE = -1e30
SUB = 8
CHUNK = 512
UNROLL = 4

VMEM = pl.BlockSpec(memory_space=pltpu.VMEM)
SMEM = pl.BlockSpec(memory_space=pltpu.SMEM)


def fill_holders(holders, order_ref, count, window):
    for i in range(window):
        holders[i] = -1
        holders[count + window + i] = -1
    for c in range(count):
        holders[order_ref[0, c] + window] = c


def spread_kernel(head_ref, mask_ref, rows_ref, out_ref, *, heads):
    pieces = out_ref.shape[0]
    group = 256
    tokens = group // heads
    row = lax.broadcasted_iota(jnp.int32, (tokens, group), 1)
    token = lax.broadcasted_iota(jnp.int32, (tokens, group), 0)
    chosen = (row == token * heads + head_ref[0]).astype(jnp.float32).astype(jnp.bfloat16)
    each = tokens // SUB
    counted = jnp.sum(mask_ref[...].astype(jnp.float32), axis=1, keepdims=True)
    counted = jnp.broadcast_to(counted, (SUB, out_ref.shape[2])).astype(out_ref.dtype)
    for n in range(pieces // each):
        picked = jnp.dot(
            chosen, rows_ref[n * group : (n + 1) * group], preferred_element_type=jnp.float32
        ).astype(out_ref.dtype)
        for e in range(each):
            out_ref[n * each + e, :SUB] = picked[e * SUB : (e + 1) * SUB]
            out_ref[n * each + e, SUB:] = counted


def select_kernel(
    order_ref, length_ref, got_ref, out_ref, count_ref, edge_ref, holders, *, count, window
):
    fill_holders(holders, order_ref, count, window)
    total = jnp.zeros((SUB, got_ref.shape[2]), jnp.float32)
    for c in range(count):
        total = total + got_ref[c, SUB:].astype(jnp.float32)
    count_ref[...] = total
    docs = length_ref.shape[1]
    lane = lax.broadcasted_iota(jnp.int32, (1, got_ref.shape[2]), 1)
    first = jnp.where(lane == docs, -(window + 1) * got_ref.shape[2], 0)
    last = jnp.zeros_like(first)
    running = jnp.int32(0)
    for d in range(docs):
        first = jnp.where(lane == d, running, first)
        running = running + length_ref[0, d]
        last = jnp.where(lane == d, running, last)
    edge_ref[0:1] = first
    edge_ref[1:2] = last
    for d in range(count):
        own = order_ref[0, d]
        for j in range(window):
            source = jnp.maximum(holders[own + j], 0)
            out_ref[d, j] = got_ref[source, :SUB]


def reduce_kernel(
    order_ref, count_ref, got_ref, rows_ref, out_ref, grad_ref, holders, *, count, window, groups, tokens
):
    fill_holders(holders, order_ref, count, window)
    total = count_ref[:1]
    for k in range(groups - 1):
        other = got_ref[k, window + 1].astype(jnp.float32)
        total = total + other[:1] * 64.0 + other[4:5]
    weight = tokens / jnp.maximum(total, 1.0)
    copies = out_ref.shape[1]
    for c in range(count):
        own = order_ref[0, c]
        summed = got_ref[c, window].astype(jnp.float32)
        for j in range(window):
            source = holders[own + 2 * window - j]
            term = got_ref[jnp.maximum(source, 0), j].astype(jnp.float32)
            summed = summed + jnp.where(source >= 0, term, 0.0)
        piece = (summed * weight).astype(out_ref.dtype)
        for g in range(copies):
            out_ref[c, g] = piece
    grad_ref[...] = (rows_ref[...] * weight).astype(grad_ref.dtype)


def attend_kernel(
    me_ref,
    order_ref,
    mask_ref,
    edge_ref,
    q_ref,
    up_ref,
    own_ref,
    got_ref,
    count_ref,
    att_ref,
    gq_ref,
    part_ref,
    keys,
    values,
    keys_t,
    values_t,
    grad_k,
    grad_v,
    *,
    window,
    heads,
    chunk,
    unroll,
):
    pieces = own_ref.shape[0]
    half = pieces // 2
    rows, width = q_ref.shape
    block = half * SUB
    prior = window * block
    span = prior + block
    factor = 1.0 / math.sqrt(width)
    own = order_ref[0, me_ref[0]]
    first = edge_ref[0:1]
    last = edge_ref[1:2]

    for j in range(window):
        keys[j * block : (j + 1) * block, :width] = got_ref[:half, j].reshape(block, width)
        values[j * block : (j + 1) * block] = got_ref[half:, j].reshape(block, width)
    keys[prior:, :width] = own_ref[:half, :SUB].reshape(block, width)
    values[prior:] = own_ref[half:, :SUB].reshape(block, width)
    spot = (own - window) * block + lax.broadcasted_iota(jnp.int32, (span, width), 0)
    within = (spot >= first) & (spot < last)
    keys[:, width:] = jnp.where(within, 1.0, 0.0).astype(jnp.bfloat16)
    keys_t[...] = keys[:, :width].astype(jnp.float32).T.astype(jnp.bfloat16)
    values_t[...] = values[...].astype(jnp.float32).T.astype(jnp.bfloat16)
    grad_k[...] = jnp.zeros_like(grad_k)
    grad_v[...] = jnp.zeros_like(grad_v)

    nt = (((1,), (1,)), ((), ()))
    nn = (((1,), (0,)), ((), ()))

    def dot(a, b, dims):
        return lax.dot_general(a, b, dims, preferred_element_type=jnp.float32)

    assert heads & (heads - 1) == 0

    def token_of(row):
        return lax.shift_right_logical(row, heads.bit_length() - 1)

    def step(c, _):
        start = pl.multiple_of(c * chunk, chunk)
        here = pl.ds(start, chunk)
        q = q_ref[here, :]
        place = own * block + token_of(start + lax.broadcasted_iota(jnp.int32, (chunk, width), 0))
        within = (place >= first) & (place < last)
        barred = jnp.where(within, 0.0, FLOOR_SCORE).astype(jnp.bfloat16)
        token = token_of(start)
        up = jnp.concatenate(
            [
                up_ref[pl.ds(start + i * heads, heads), :]
                * mask_ref[0, token + i].astype(jnp.float32).astype(jnp.bfloat16)
                for i in range(chunk // heads)
            ],
            axis=0,
        )

        scores = dot(keys[...], jnp.concatenate([q, barred], axis=1), nt)
        index = lax.broadcasted_iota(jnp.int32, (block, chunk), 0)
        column = token_of(start + lax.broadcasted_iota(jnp.int32, (block, chunk), 1))
        here_scores = jnp.where(index <= column, scores[prior:], FLOOR_SCORE)
        scores = jnp.concatenate([scores[:prior], here_scores], axis=0)
        highest = jnp.max(scores, axis=0, keepdims=True)
        exponent = jnp.exp2((scores - highest) * (factor / math.log(2.0)))
        probs = exponent * (1.0 / jnp.sum(exponent, axis=0, keepdims=True))
        probs_low = probs.astype(jnp.bfloat16)
        prob_grad = dot(values[...], up, nt)
        att = dot(values_t[...], probs_low, nn)
        att_ref[here, :] = att.T.astype(att_ref.dtype)
        delta = jnp.sum(probs * prob_grad, axis=0, keepdims=True)
        score_grad = (probs * (prob_grad - delta)).astype(jnp.bfloat16)
        gq = dot(keys_t[...], score_grad, nn)
        gq_ref[here, :] = gq.T * factor
        grad_v[...] += dot(probs_low, up, nn)
        grad_k[...] += dot(score_grad, q, nn)
        return 0

    lax.fori_loop(0, rows // chunk, step, 0, unroll=unroll)

    for j in range(window + 1):
        part_ref[:half, j] = (
            (grad_k[j * block : (j + 1) * block] * factor)
            .astype(part_ref.dtype)
            .reshape(half, SUB, width)
        )
        part_ref[half:, j] = (
            grad_v[j * block : (j + 1) * block]
            .astype(part_ref.dtype)
            .reshape(half, SUB, width)
        )
    high = jnp.floor(count_ref[...] * (1.0 / 64.0))
    low = count_ref[...] - high * 64.0
    upper = lax.broadcasted_iota(jnp.int32, (SUB, width), 0) < 4
    halves = jnp.where(upper, high, low).astype(part_ref.dtype)
    for i in range(pieces):
        part_ref[i, window + 1] = halves


def limit(mib):
    return pltpu.CompilerParams(vmem_limit_bytes=mib * 1024 * 1024)


def exchange(x, axes):
    return lax.all_to_all(x, axes, 0, 0, tiled=True)


def local(query, key_value, grad_out, doc_lengths, stretch_order, loss_mask):
    shard_rows, local_heads, head_width = query.shape[1:]
    kv_heads = key_value.shape[3]
    count = lax.axis_size(CTX)
    length = shard_rows * count
    longest = length * 5 // 32
    window = (longest - 1 + shard_rows - 1) // shard_rows
    rows = shard_rows * local_heads
    tokens = float(lax.axis_size(DP) * query.shape[0] * length)
    pieces = 2 * shard_rows // SUB
    assert pieces == count

    head = lax.axis_index("tensor").reshape(1).astype(jnp.int32)
    spread = pl.pallas_call(
        functools.partial(spread_kernel, heads=kv_heads),
        out_shape=jax.ShapeDtypeStruct((pieces, 2 * SUB, head_width), jnp.bfloat16),
        in_specs=[SMEM, VMEM, VMEM],
        out_specs=VMEM,
        compiler_params=limit(4),
        cost_estimate=pl.CostEstimate(flops=20_000_000, bytes_accessed=700_000, transcendentals=0),
        name="spread",
    )(head, loss_mask, key_value.reshape(2 * shard_rows * kv_heads, head_width))
    got = exchange(spread, CTX)

    chosen, counted, edges = pl.pallas_call(
        functools.partial(select_kernel, count=count, window=window),
        out_shape=(
            jax.ShapeDtypeStruct((count, window, SUB, head_width), jnp.bfloat16),
            jax.ShapeDtypeStruct((SUB, head_width), jnp.float32),
            jax.ShapeDtypeStruct((SUB, head_width), jnp.int32),
        ),
        in_specs=[SMEM, SMEM, VMEM],
        out_specs=(VMEM, VMEM, VMEM),
        scratch_shapes=[pltpu.SMEM((count + 2 * window,), jnp.int32)],
        compiler_params=limit(4),
        cost_estimate=pl.CostEstimate(flops=2_000_000, bytes_accessed=500_000, transcendentals=0),
        name="select",
    )(stretch_order, doc_lengths, got)
    groups = lax.axis_size(DP)
    pairs = [
        (a * count + c, (a ^ (1 + c % (groups - 1))) * count + c)
        for a in range(groups)
        for c in range(count)
    ]
    heard = lax.ppermute(counted, DP + CTX, pairs)
    fetched = exchange(chosen.reshape(count, window * SUB, head_width), CTX)
    fetched = fetched.reshape(count, window, SUB, head_width)

    me = lax.axis_index(CTX).reshape(1).astype(jnp.int32)
    span = (window + 1) * shard_rows
    attended, grad_rows, parts = pl.pallas_call(
        functools.partial(
            attend_kernel, window=window, heads=local_heads, chunk=CHUNK, unroll=UNROLL
        ),
        out_shape=(
            jax.ShapeDtypeStruct((rows, head_width), jnp.bfloat16),
            jax.ShapeDtypeStruct((rows, head_width), jnp.float32),
            jax.ShapeDtypeStruct((count, window + 2, SUB, head_width), jnp.bfloat16),
        ),
        in_specs=[SMEM, SMEM, SMEM, VMEM, VMEM, VMEM, VMEM, VMEM, VMEM],
        out_specs=(VMEM, VMEM, VMEM),
        scratch_shapes=[
            pltpu.VMEM((span, 2 * head_width), jnp.bfloat16),
            pltpu.VMEM((span, head_width), jnp.bfloat16),
            pltpu.VMEM((head_width, span), jnp.bfloat16),
            pltpu.VMEM((head_width, span), jnp.bfloat16),
            pltpu.VMEM((span, head_width), jnp.float32),
            pltpu.VMEM((span, head_width), jnp.float32),
        ],
        compiler_params=limit(24),
        cost_estimate=pl.CostEstimate(
            flops=12 * rows * span * head_width, bytes_accessed=4_000_000, transcendentals=rows * span
        ),
        name="attend",
    )(
        me,
        stretch_order,
        loss_mask,
        edges,
        query.reshape(rows, head_width),
        grad_out.reshape(rows, head_width),
        spread,
        fetched,
        heard,
    )

    met = exchange(parts.reshape(count, (window + 2) * SUB, head_width), CTX)
    summed, grad_query = pl.pallas_call(
        functools.partial(
            reduce_kernel, count=count, window=window, groups=groups, tokens=tokens
        ),
        out_shape=(
            jax.ShapeDtypeStruct((count, kv_heads, SUB, head_width), jnp.bfloat16),
            jax.ShapeDtypeStruct((rows, head_width), jnp.bfloat16),
        ),
        in_specs=[SMEM, VMEM, VMEM, VMEM],
        out_specs=(VMEM, VMEM),
        scratch_shapes=[pltpu.SMEM((count + 2 * window,), jnp.int32)],
        compiler_params=limit(6),
        cost_estimate=pl.CostEstimate(flops=2_000_000, bytes_accessed=1_000_000, transcendentals=0),
        name="reduce",
    )(stretch_order, counted, met.reshape(count, window + 2, SUB, head_width), grad_rows)
    home = exchange(summed.reshape(count * kv_heads, SUB, head_width), WORLD)
    home = home.reshape(2, pieces // 2, kv_heads, SUB, head_width)
    grad_key_value = jnp.transpose(home, (0, 1, 3, 2, 4)).reshape(
        2, 1, shard_rows, kv_heads, head_width
    )
    return (attended.reshape(query.shape), grad_query.reshape(query.shape), grad_key_value)


def solution(mesh):
    torus = Mesh(
        mesh.devices.reshape(2, 2, 8, 4, mesh.shape["tensor"]),
        ("dp_0", "dp_1", "ctx_0", "ctx_1", "tensor"),
    )
    placed = (
        P(DP, CTX, "tensor", None),
        P(None, DP, CTX, None, None),
        P(DP, CTX, "tensor", None),
        P(DP, None),
        P(DP, None),
        P(DP, CTX),
    )
    return jax.shard_map(
        local,
        mesh=torus,
        in_specs=placed,
        out_specs=(
            P(DP, CTX, "tensor", None),
            P(DP, CTX, "tensor", None),
            P(None, DP, CTX, None, None),
        ),
        check_vma=False,
    )
```

```python
import functools
import math

import jax
import jax.numpy as jnp
from jax import lax
from jax.experimental import pallas as pl
from jax.experimental.pallas import tpu as pltpu
from jax.sharding import Mesh
from jax.sharding import PartitionSpec as P

CTX = ("ctx_0", "ctx_1")
DP = ("dp_0", "dp_1")
WORLD = ("ctx_0", "ctx_1", "tensor")

FLOOR_SCORE = -1e30
SUB = 8
CHUNK = 512
UNROLL = 4

VMEM = pl.BlockSpec(memory_space=pltpu.VMEM)
SMEM = pl.BlockSpec(memory_space=pltpu.SMEM)


def fill_holders(holders, order_ref, count, window):
    for i in range(window):
        holders[i] = -1
        holders[count + window + i] = -1
    for c in range(count):
        holders[order_ref[0, c] + window] = c


def spread_kernel(head_ref, mask_ref, rows_ref, out_ref, *, heads):
    pieces = out_ref.shape[0]
    group = 256
    tokens = group // heads
    row = lax.broadcasted_iota(jnp.int32, (tokens, group), 1)
    token = lax.broadcasted_iota(jnp.int32, (tokens, group), 0)
    chosen = (row == token * heads + head_ref[0]).astype(jnp.float32).astype(jnp.bfloat16)
    each = tokens // SUB
    counted = jnp.sum(mask_ref[...].astype(jnp.float32), axis=1, keepdims=True)
    counted = jnp.broadcast_to(counted, (SUB, out_ref.shape[2])).astype(out_ref.dtype)
    for n in range(pieces // each):
        picked = jnp.dot(
            chosen, rows_ref[n * group : (n + 1) * group], preferred_element_type=jnp.float32
        ).astype(out_ref.dtype)
        for e in range(each):
            out_ref[n * each + e, :SUB] = picked[e * SUB : (e + 1) * SUB]
            out_ref[n * each + e, SUB:] = counted


def select_kernel(
    order_ref, length_ref, got_ref, out_ref, count_ref, edge_ref, holders, *, count, window
):
    fill_holders(holders, order_ref, count, window)
    total = jnp.zeros((SUB, got_ref.shape[2]), jnp.float32)
    for c in range(count):
        total = total + got_ref[c, SUB:].astype(jnp.float32)
    for k in range(count_ref.shape[0]):
        count_ref[k] = total
    docs = length_ref.shape[1]
    lane = lax.broadcasted_iota(jnp.int32, (1, got_ref.shape[2]), 1)
    first = jnp.where(lane == docs, -(window + 1) * got_ref.shape[2], 0)
    last = jnp.zeros_like(first)
    running = jnp.int32(0)
    for d in range(docs):
        first = jnp.where(lane == d, running, first)
        running = running + length_ref[0, d]
        last = jnp.where(lane == d, running, last)
    edge_ref[0:1] = first
    edge_ref[1:2] = last
    for d in range(count):
        own = order_ref[0, d]
        for j in range(window):
            source = jnp.maximum(holders[own + j], 0)
            out_ref[d, j] = got_ref[source, :SUB]


def reduce_kernel(
    order_ref, count_ref, got_ref, rows_ref, out_ref, grad_ref, holders, *, count, window, tokens
):
    fill_holders(holders, order_ref, count, window)
    total = count_ref[0, :1]
    for k in range(1, count_ref.shape[0]):
        total = total + count_ref[k, :1]
    weight = tokens / jnp.maximum(total, 1.0)
    copies = out_ref.shape[1]
    for c in range(count):
        own = order_ref[0, c]
        summed = got_ref[c, window].astype(jnp.float32)
        for j in range(window):
            source = holders[own + 2 * window - j]
            term = got_ref[jnp.maximum(source, 0), j].astype(jnp.float32)
            summed = summed + jnp.where(source >= 0, term, 0.0)
        piece = (summed * weight).astype(out_ref.dtype)
        for g in range(copies):
            out_ref[c, g] = piece
    grad_ref[...] = (rows_ref[...] * weight).astype(grad_ref.dtype)


def attend_kernel(
    me_ref,
    order_ref,
    mask_ref,
    edge_ref,
    q_ref,
    up_ref,
    own_ref,
    got_ref,
    att_ref,
    gq_ref,
    part_ref,
    keys,
    values,
    keys_t,
    values_t,
    grad_k,
    grad_v,
    *,
    window,
    heads,
    chunk,
    unroll,
):
    pieces = own_ref.shape[0]
    half = pieces // 2
    rows, width = q_ref.shape
    block = half * SUB
    prior = window * block
    span = prior + block
    factor = 1.0 / math.sqrt(width)
    own = order_ref[0, me_ref[0]]
    first = edge_ref[0:1]
    last = edge_ref[1:2]

    for j in range(window):
        keys[j * block : (j + 1) * block, :width] = got_ref[:half, j].reshape(block, width)
        values[j * block : (j + 1) * block] = got_ref[half:, j].reshape(block, width)
    keys[prior:, :width] = own_ref[:half, :SUB].reshape(block, width)
    values[prior:] = own_ref[half:, :SUB].reshape(block, width)
    spot = (own - window) * block + lax.broadcasted_iota(jnp.int32, (span, width), 0)
    within = (spot >= first) & (spot < last)
    keys[:, width:] = jnp.where(within, 1.0, 0.0).astype(jnp.bfloat16)
    keys_t[...] = keys[:, :width].astype(jnp.float32).T.astype(jnp.bfloat16)
    values_t[...] = values[...].astype(jnp.float32).T.astype(jnp.bfloat16)
    grad_k[...] = jnp.zeros_like(grad_k)
    grad_v[...] = jnp.zeros_like(grad_v)

    nt = (((1,), (1,)), ((), ()))
    nn = (((1,), (0,)), ((), ()))

    def dot(a, b, dims):
        return lax.dot_general(a, b, dims, preferred_element_type=jnp.float32)

    assert heads & (heads - 1) == 0

    def token_of(row):
        return lax.shift_right_logical(row, heads.bit_length() - 1)

    def step(c, _):
        start = pl.multiple_of(c * chunk, chunk)
        here = pl.ds(start, chunk)
        q = q_ref[here, :]
        place = own * block + token_of(start + lax.broadcasted_iota(jnp.int32, (chunk, width), 0))
        within = (place >= first) & (place < last)
        barred = jnp.where(within, 0.0, FLOOR_SCORE).astype(jnp.bfloat16)
        token = token_of(start)
        up = jnp.concatenate(
            [
                up_ref[pl.ds(start + i * heads, heads), :]
                * mask_ref[0, token + i].astype(jnp.float32).astype(jnp.bfloat16)
                for i in range(chunk // heads)
            ],
            axis=0,
        )

        scores = dot(keys[...], jnp.concatenate([q, barred], axis=1), nt)
        index = lax.broadcasted_iota(jnp.int32, (block, chunk), 0)
        column = token_of(start + lax.broadcasted_iota(jnp.int32, (block, chunk), 1))
        here_scores = jnp.where(index <= column, scores[prior:], FLOOR_SCORE)
        scores = jnp.concatenate([scores[:prior], here_scores], axis=0)
        highest = jnp.max(scores, axis=0, keepdims=True)
        exponent = jnp.exp2((scores - highest) * (factor / math.log(2.0)))
        probs = exponent * (1.0 / jnp.sum(exponent, axis=0, keepdims=True))
        probs_low = probs.astype(jnp.bfloat16)
        prob_grad = dot(values[...], up, nt)
        att = dot(values_t[...], probs_low, nn)
        att_ref[here, :] = att.T.astype(att_ref.dtype)
        delta = jnp.sum(probs * prob_grad, axis=0, keepdims=True)
        score_grad = (probs * (prob_grad - delta)).astype(jnp.bfloat16)
        gq = dot(keys_t[...], score_grad, nn)
        gq_ref[here, :] = gq.T * factor
        grad_v[...] += dot(probs_low, up, nn)
        grad_k[...] += dot(score_grad, q, nn)
        return 0

    lax.fori_loop(0, rows // chunk, step, 0, unroll=unroll)

    for j in range(window + 1):
        part_ref[:half, j] = (
            (grad_k[j * block : (j + 1) * block] * factor)
            .astype(part_ref.dtype)
            .reshape(half, SUB, width)
        )
        part_ref[half:, j] = (
            grad_v[j * block : (j + 1) * block]
            .astype(part_ref.dtype)
            .reshape(half, SUB, width)
        )


def limit(mib):
    return pltpu.CompilerParams(vmem_limit_bytes=mib * 1024 * 1024)


def exchange(x, axes):
    return lax.all_to_all(x, axes, 0, 0, tiled=True)


def local(query, key_value, grad_out, doc_lengths, stretch_order, loss_mask):
    shard_rows, local_heads, head_width = query.shape[1:]
    kv_heads = key_value.shape[3]
    count = lax.axis_size(CTX)
    length = shard_rows * count
    longest = length * 5 // 32
    window = (longest - 1 + shard_rows - 1) // shard_rows
    rows = shard_rows * local_heads
    tokens = float(lax.axis_size(DP) * query.shape[0] * length)
    pieces = 2 * shard_rows // SUB
    assert pieces == count

    head = lax.axis_index("tensor").reshape(1).astype(jnp.int32)
    spread = pl.pallas_call(
        functools.partial(spread_kernel, heads=kv_heads),
        out_shape=jax.ShapeDtypeStruct((pieces, 2 * SUB, head_width), jnp.bfloat16),
        in_specs=[SMEM, VMEM, VMEM],
        out_specs=VMEM,
        compiler_params=limit(4),
        cost_estimate=pl.CostEstimate(flops=20_000_000, bytes_accessed=700_000, transcendentals=0),
        name="spread",
    )(head, loss_mask, key_value.reshape(2 * shard_rows * kv_heads, head_width))
    got = exchange(spread, CTX)

    groups = lax.axis_size(DP)
    chosen, counted, edges = pl.pallas_call(
        functools.partial(select_kernel, count=count, window=window),
        out_shape=(
            jax.ShapeDtypeStruct((count, window, SUB, head_width), jnp.bfloat16),
            jax.ShapeDtypeStruct((groups, SUB, head_width), jnp.float32),
            jax.ShapeDtypeStruct((SUB, head_width), jnp.int32),
        ),
        in_specs=[SMEM, SMEM, VMEM],
        out_specs=(VMEM, VMEM, VMEM),
        scratch_shapes=[pltpu.SMEM((count + 2 * window,), jnp.int32)],
        compiler_params=limit(4),
        cost_estimate=pl.CostEstimate(flops=2_000_000, bytes_accessed=500_000, transcendentals=0),
        name="select",
    )(stretch_order, doc_lengths, got)
    fetched = exchange(chosen.reshape(count, window * SUB, head_width), CTX)
    counted, fetched = lax.optimization_barrier((counted, fetched))
    told = exchange(counted, DP)
    fetched = fetched.reshape(count, window, SUB, head_width)

    me = lax.axis_index(CTX).reshape(1).astype(jnp.int32)
    span = (window + 1) * shard_rows
    attended, grad_rows, parts = pl.pallas_call(
        functools.partial(
            attend_kernel, window=window, heads=local_heads, chunk=CHUNK, unroll=UNROLL
        ),
        out_shape=(
            jax.ShapeDtypeStruct((rows, head_width), jnp.bfloat16),
            jax.ShapeDtypeStruct((rows, head_width), jnp.float32),
            jax.ShapeDtypeStruct((count, window + 1, SUB, head_width), jnp.bfloat16),
        ),
        in_specs=[SMEM, SMEM, SMEM, VMEM, VMEM, VMEM, VMEM, VMEM],
        out_specs=(VMEM, VMEM, VMEM),
        scratch_shapes=[
            pltpu.VMEM((span, 2 * head_width), jnp.bfloat16),
            pltpu.VMEM((span, head_width), jnp.bfloat16),
            pltpu.VMEM((head_width, span), jnp.bfloat16),
            pltpu.VMEM((head_width, span), jnp.bfloat16),
            pltpu.VMEM((span, head_width), jnp.float32),
            pltpu.VMEM((span, head_width), jnp.float32),
        ],
        compiler_params=limit(24),
        cost_estimate=pl.CostEstimate(
            flops=12 * rows * span * head_width, bytes_accessed=4_000_000, transcendentals=rows * span
        ),
        name="attend",
    )(
        me,
        stretch_order,
        loss_mask,
        edges,
        query.reshape(rows, head_width),
        grad_out.reshape(rows, head_width),
        spread,
        fetched,
    )

    met = exchange(parts.reshape(count, (window + 1) * SUB, head_width), CTX)
    summed, grad_query = pl.pallas_call(
        functools.partial(
            reduce_kernel, count=count, window=window, tokens=tokens
        ),
        out_shape=(
            jax.ShapeDtypeStruct((count, kv_heads, SUB, head_width), jnp.bfloat16),
            jax.ShapeDtypeStruct((rows, head_width), jnp.bfloat16),
        ),
        in_specs=[SMEM, VMEM, VMEM, VMEM],
        out_specs=(VMEM, VMEM),
        scratch_shapes=[pltpu.SMEM((count + 2 * window,), jnp.int32)],
        compiler_params=limit(6),
        cost_estimate=pl.CostEstimate(flops=2_000_000, bytes_accessed=1_000_000, transcendentals=0),
        name="reduce",
    )(stretch_order, told, met.reshape(count, window + 1, SUB, head_width), grad_rows)
    home = exchange(summed.reshape(count * kv_heads, SUB, head_width), WORLD)
    home = home.reshape(2, pieces // 2, kv_heads, SUB, head_width)
    grad_key_value = jnp.transpose(home, (0, 1, 3, 2, 4)).reshape(
        2, 1, shard_rows, kv_heads, head_width
    )
    return (attended.reshape(query.shape), grad_query.reshape(query.shape), grad_key_value)


def solution(mesh):
    torus = Mesh(
        mesh.devices.reshape(2, 2, 8, 4, mesh.shape["tensor"]),
        ("dp_0", "dp_1", "ctx_0", "ctx_1", "tensor"),
    )
    placed = (
        P(DP, CTX, "tensor", None),
        P(None, DP, CTX, None, None),
        P(DP, CTX, "tensor", None),
        P(DP, None),
        P(DP, None),
        P(DP, CTX),
    )
    return jax.shard_map(
        local,
        mesh=torus,
        in_specs=placed,
        out_specs=(
            P(DP, CTX, "tensor", None),
            P(DP, CTX, "tensor", None),
            P(None, DP, CTX, None, None),
        ),
        check_vma=False,
    )
```
